16 devices in a mesh: rep: 2 (over y, z), shard: 8 (over x, core).
Axes of the slice: x: 4, y: 2, z: 1, core: 2. Of those that a mesh axis runs over, the one named last changes fastest.
The devices are a block of a 4x4x8 slice.
Arguments:
- ratings: float32 [8192, 4096], P(('rep', 'shard')), parts along dimension 0
- obs_mask: int32 [8192, 4096], P(('rep', 'shard')), parts along dimension 0
- step_counts: int32 [16, 8], P(('rep', 'shard')), parts along dimension 0
- user_init: float32 [8192, 256], P(('rep', 'shard')), parts along dimension 0
- item_init: float32 [8192, 256], P(('rep', 'shard')), parts along dimension 0
Outputs:
- output 1: float32 [8192, 256], P(('rep', 'shard')), parts along dimension 0
- output 2: float32 [8192, 256], P(('rep', 'shard')), parts along dimension 0
There are 2 independent parts. The reference program is written for one: setup_inputs(seed, part) draws one part's arguments, and reference() takes and returns one part's arrays. A program takes and returns all parts, laid end to end along the dimension named above; each array names one.
All inputs are finite; a program needn't handle non-finite values.
Results may differ from the reference program's by a relative error of at most 0.00175092.
Values are sent between devices in bfloat16 or wider.
A program may use at most 768 MiB of HBM per device.

```python
import math
import jax
import jax.numpy as jnp
from jax import lax

GROUP_SIZE = 8
FACTOR_RANK = 256
ASPECT = 1
ITEMS_DEV = 512
STEPS_MAX = 2
EPOCHS = 2

USERS_DEV = ASPECT * ITEMS_DEV
NUM_USERS = GROUP_SIZE * USERS_DEV
NUM_ITEMS = GROUP_SIZE * ITEMS_DEV
TRUE_RANK = FACTOR_RANK // 4
STEP_SIZE = 0.4 * math.sqrt(FACTOR_RANK) / (USERS_DEV + FACTOR_RANK)
DECAY_RATE = 0.1 * ITEMS_DEV / math.sqrt(FACTOR_RANK)


def draw_layout(layout_key):
    key_list = jax.random.split(layout_key, 5)
    density_pct = jax.random.randint(key_list[0], (GROUP_SIZE, 1, GROUP_SIZE, 1), 10, 41)
    coin_draws = jax.random.randint(key_list[1], (GROUP_SIZE, USERS_DEV, GROUP_SIZE, ITEMS_DEV), 0, 100)
    obs_mask = (coin_draws < density_pct).astype(jnp.int32).reshape(NUM_USERS, NUM_ITEMS)
    slot_count = GROUP_SIZE * GROUP_SIZE
    step_flat = jax.random.randint(key_list[2], (slot_count,), 1, STEPS_MAX + 1)
    top_pos = jax.random.randint(key_list[3], (), 0, slot_count)
    low_pos = (top_pos + 1 + jax.random.randint(key_list[4], (), 0, slot_count - 1)) % slot_count
    slot_ids = jnp.arange(slot_count)
    step_flat = jnp.where(slot_ids == top_pos, STEPS_MAX, jnp.where(slot_ids == low_pos, 1, step_flat))
    return obs_mask, step_flat.reshape(GROUP_SIZE, GROUP_SIZE).astype(jnp.int32)


def setup_inputs(seed: int = 0, part: int = 0) -> dict:
    base_key = jax.random.fold_in(jax.random.key(seed), part)
    key_list = jax.random.split(base_key, 6)
    user_true = jax.random.normal(key_list[0], (NUM_USERS, TRUE_RANK), jnp.float32)
    item_true = jax.random.normal(key_list[1], (NUM_ITEMS, TRUE_RANK), jnp.float32)
    noise_term = 0.3 * jax.random.normal(key_list[2], (NUM_USERS, NUM_ITEMS), jnp.float32)
    ratings = jnp.dot(user_true, item_true.T) / math.sqrt(TRUE_RANK) + noise_term
    obs_mask, step_counts = draw_layout(key_list[3])
    factor_scale = FACTOR_RANK ** -0.25
    user_init = factor_scale * jax.random.normal(key_list[4], (NUM_USERS, FACTOR_RANK), jnp.float32)
    item_init = factor_scale * jax.random.normal(key_list[5], (NUM_ITEMS, FACTOR_RANK), jnp.float32)
    return {"ratings": ratings, "obs_mask": obs_mask, "step_counts": step_counts, "user_init": user_init, "item_init": item_init}


def reference(ratings, obs_mask, step_counts, user_init, item_init):
    rating_blocks = ratings.reshape(GROUP_SIZE, USERS_DEV, GROUP_SIZE, ITEMS_DEV)
    mask_blocks = obs_mask.reshape(GROUP_SIZE, USERS_DEV, GROUP_SIZE, ITEMS_DEV)
    user_blocks = user_init.reshape(GROUP_SIZE, USERS_DEV, FACTOR_RANK)
    item_blocks = item_init.reshape(GROUP_SIZE, ITEMS_DEV, FACTOR_RANK)
    row_ids = jnp.arange(GROUP_SIZE)

    def block_update(block_args):
        row_id, col_id, user_blk, item_blk = block_args
        rating_blk = rating_blocks[row_id, :, col_id, :]
        seen_blk = mask_blocks[row_id, :, col_id, :] != 0

        def grad_step(step_idx, inner_in):
            user_now, item_now = inner_in
            user_half = user_now.astype(jnp.bfloat16)
            item_half = item_now.astype(jnp.bfloat16)
            approx = jnp.dot(user_half, item_half.T, preferred_element_type=jnp.float32)
            err_half = jnp.where(seen_blk, approx - rating_blk, 0.0).astype(jnp.bfloat16)
            grad_user = jnp.dot(err_half, item_half, preferred_element_type=jnp.float32) + DECAY_RATE * user_now
            grad_item = jnp.dot(err_half.T, user_half, preferred_element_type=jnp.float32) + DECAY_RATE * item_now
            return user_now - STEP_SIZE * grad_user, item_now - STEP_SIZE * grad_item

        return lax.fori_loop(0, step_counts[row_id, col_id], grad_step, (user_blk, item_blk))

    def sub_epoch(sweep_idx, carry_in):
        user_cur, held_items = carry_in
        col_ids = (row_ids + sweep_idx) % GROUP_SIZE
        user_new, item_new = lax.map(block_update, (row_ids, col_ids, user_cur, held_items))
        return user_new, jnp.roll(item_new, -1, axis=0)

    user_fin, item_fin = lax.fori_loop(0, EPOCHS * GROUP_SIZE, sub_epoch, (user_blocks, item_blocks))
    return user_fin.reshape(NUM_USERS, FACTOR_RANK), item_fin.reshape(NUM_ITEMS, FACTOR_RANK)
```

```python
import functools
import math
import jax
import jax.numpy as jnp
from jax import lax
from jax.experimental import pallas as pl
from jax.experimental.pallas import tpu as pltpu
from jax.sharding import PartitionSpec as P

EPOCHS = 2
CHUNKS = 2
ROWS = 256
F32 = jnp.float32
BF16 = jnp.bfloat16
MESH = pl.DeviceIdType.MESH


def dot_nn(lhs, rhs):
    return jnp.dot(lhs, rhs, preferred_element_type=F32)


def dot_nt(lhs, rhs):
    return lax.dot_general(lhs, rhs, (((1,), (1,)), ((), ())), preferred_element_type=F32)


def sgd_kernel(group, axis, steps_ref, user_ref, item_ref, ratings_ref, mask_ref, user_out, item_out,
               rate_v, seen_v, vin, vout, v_mid, user_v, user_h, user_t, grad_u, err_v,
               rate_sem, seen_sem, send_sem, recv_sem):
    users, rank = user_ref.shape
    items = item_ref.shape[0]
    width = items // CHUNKS
    levels = EPOCHS * group
    eta = 0.4 * math.sqrt(rank) / (users + rank)
    lam = 0.1 * items / math.sqrt(rank)
    me = lax.axis_index(axis)
    left = lax.rem(me + group - 1, group)
    right = lax.rem(me + 1, group)

    def load(sweep):
        col = lax.rem(me + sweep, group)
        src = pl.ds(pl.multiple_of(col * items, items), items)
        return (
            pltpu.make_async_copy(ratings_ref.at[:, src], rate_v.at[col], rate_sem.at[sweep]),
            pltpu.make_async_copy(mask_ref.at[:, src], seen_v.at[col], seen_sem.at[sweep]),
        )

    def hop(sweep, k):
        return pltpu.make_async_remote_copy(
            src_ref=vout.at[sweep, k],
            dst_ref=vin.at[sweep + 1, k],
            send_sem=send_sem.at[sweep, k],
            recv_sem=recv_sem.at[sweep, k],
            device_id={axis: left},
            device_id_type=MESH,
        )

    for sweep in range(group):
        for copy in load(sweep):
            copy.start()

    barrier = pltpu.get_barrier_semaphore()
    for other in (left, right):
        pl.semaphore_signal(barrier, inc=1, device_id={axis: other}, device_id_type=MESH)

    def put_user(value):
        user_v[...] = value
        half = value.astype(BF16)
        user_h[...] = half
        user_t[...] = half.T

    put_user(user_ref[...])
    for k in range(CHUNKS):
        vin[0, k] = item_ref[k * width:(k + 1) * width, :].T
    pl.semaphore_wait(barrier, 2)

    def grad_step(col, k, v_now):
        half = v_now.astype(BF16)
        for row in range(0, users, ROWS):
            rows = slice(row, row + ROWS)
            cols = slice(k * width, (k + 1) * width)
            approx = dot_nn(user_h[rows, :], half)
            err = jnp.where(seen_v[col, rows, cols] != 0, approx - rate_v[col, rows, cols], 0.0).astype(BF16)
            err_v[rows, :] = err
            part = dot_nt(err, half)
            if k == 0:
                grad_u[rows, :] = part
            else:
                grad_u[rows, :] += part
        grad_v = dot_nn(user_t[...], err_v[...])
        return v_now - eta * (grad_v + lam * v_now)

    def level(sweep, carry):
        col = lax.rem(me + sweep, group)
        twice = steps_ref[0, col] > 1

        @pl.when(sweep < group)
        def _():
            for copy in load(sweep):
                copy.wait()

        for k in range(CHUNKS):
            @pl.when(sweep > 0)
            def _():
                hop(sweep - 1, k).wait_recv()

            v_mid[k] = grad_step(col, k, vin[sweep, k])
        user_now = user_v[...]
        put_user(user_now - eta * (grad_u[...] + lam * user_now))
        for k in range(CHUNKS):
            v_now = v_mid[k]
            v_new = grad_step(col, k, v_now)
            vout[sweep, k] = jnp.where(twice, v_new, v_now)
            hop(sweep, k).start()
        user_now = user_v[...]
        user_new = user_now - eta * (grad_u[...] + lam * user_now)
        put_user(jnp.where(twice, user_new, user_now))
        return carry

    lax.fori_loop(0, levels, level, 0)

    user_out[...] = user_v[...]
    for k in range(CHUNKS):
        hop(levels - 1, k).wait_recv()
        item_out[k * width:(k + 1) * width, :] = vin[levels, k].T

    def drain(sweep, carry):
        for k in range(CHUNKS):
            hop(sweep, k).wait_send()
        return carry

    lax.fori_loop(0, levels, drain, 0)


def solution(mesh):
    axis = "shard"
    group = mesh.shape[axis]
    row_spec = P(("rep", axis), None)
    levels = EPOCHS * group

    def local_run(ratings, obs_mask, step_counts, user_init, item_init):
        users, rank = user_init.shape
        items = item_init.shape[0]
        width = items // CHUNKS
        vmem = pl.BlockSpec(memory_space=pltpu.VMEM)
        hbm = pl.BlockSpec(memory_space=pl.ANY)
        return pl.pallas_call(
            functools.partial(sgd_kernel, group, axis),
            name="sgd",
            out_shape=(
                jax.ShapeDtypeStruct((users, rank), F32),
                jax.ShapeDtypeStruct((items, rank), F32),
            ),
            in_specs=[pl.BlockSpec(memory_space=pltpu.SMEM), vmem, vmem, hbm, hbm],
            out_specs=(vmem, vmem),
            scratch_shapes=[
                pltpu.VMEM((group, users, items), F32),
                pltpu.VMEM((group, users, items), jnp.int32),
                pltpu.VMEM((levels + 1, CHUNKS, rank, width), F32),
                pltpu.VMEM((levels, CHUNKS, rank, width), F32),
                pltpu.VMEM((CHUNKS, rank, width), F32),
                pltpu.VMEM((users, rank), F32),
                pltpu.VMEM((users, rank), BF16),
                pltpu.VMEM((rank, users), BF16),
                pltpu.VMEM((users, rank), F32),
                pltpu.VMEM((users, width), BF16),
                pltpu.SemaphoreType.DMA((group,)),
                pltpu.SemaphoreType.DMA((group,)),
                pltpu.SemaphoreType.DMA((levels, CHUNKS)),
                pltpu.SemaphoreType.DMA((levels, CHUNKS)),
            ],
            compiler_params=pltpu.CompilerParams(
                collective_id=0, has_side_effects=True, vmem_limit_bytes=60 * 1024 * 1024
            ),
        )(step_counts, user_init, item_init, ratings, obs_mask)

    return jax.shard_map(local_run, mesh=mesh, in_specs=(row_spec,) * 5, out_specs=(row_spec, row_spec), check_vma=False)
```

```python
import functools
import math
import jax
import jax.numpy as jnp
from jax import lax
from jax.experimental import pallas as pl
from jax.experimental.pallas import tpu as pltpu
from jax.sharding import PartitionSpec as P

EPOCHS = 2
CHUNKS = 2
ROWS = 256
F32 = jnp.float32
BF16 = jnp.bfloat16
MESH = pl.DeviceIdType.MESH


def dot_nn(lhs, rhs):
    return jnp.dot(lhs, rhs, preferred_element_type=F32)


def dot_nt(lhs, rhs):
    return lax.dot_general(lhs, rhs, (((1,), (1,)), ((), ())), preferred_element_type=F32)


def sgd_kernel(group, axis, steps_ref, user_ref, item_ref, ratings_ref, mask_ref, user_out, item_out,
               rate_v, seen_v, vin, vout, v_mid, item_v, user_v, user_h, user_t, grad_u, err_v,
               rate_sem, seen_sem, send_sem, recv_sem, side_sem):
    users, rank = user_ref.shape
    items = item_ref.shape[0]
    width = items // CHUNKS
    levels = EPOCHS * group
    eta = 0.4 * math.sqrt(rank) / (users + rank)
    lam = 0.1 * items / math.sqrt(rank)
    me = lax.axis_index(axis)
    left = lax.rem(me + group - 1, group)
    right = lax.rem(me + 1, group)

    def load(sweep):
        col = lax.rem(me + sweep, group)
        src = pl.ds(pl.multiple_of(col * items, items), items)
        return (
            pltpu.make_async_copy(ratings_ref.at[:, src], rate_v.at[col], rate_sem.at[sweep]),
            pltpu.make_async_copy(mask_ref.at[:, src], seen_v.at[col], seen_sem.at[sweep]),
        )

    def hop(sweep, k):
        return pltpu.make_async_remote_copy(
            src_ref=vout.at[sweep, k],
            dst_ref=vin.at[sweep + 1, k],
            send_sem=send_sem.at[sweep, k],
            recv_sem=recv_sem.at[sweep, k],
            device_id={axis: left},
            device_id_type=MESH,
        )

    user_in = pltpu.make_async_copy(user_ref, user_v, side_sem.at[0])
    item_in = pltpu.make_async_copy(item_ref, item_v, side_sem.at[1])
    for copy in (user_in, item_in, *load(0)):
        copy.start()
    barrier = pltpu.get_barrier_semaphore()
    for other in (left, right):
        pl.semaphore_signal(barrier, inc=1, device_id={axis: other}, device_id_type=MESH)

    def put_user(value):
        user_v[...] = value
        half = value.astype(BF16)
        user_h[...] = half
        user_t[...] = half.T

    user_in.wait()
    put_user(user_v[...])
    item_in.wait()
    for k in range(CHUNKS):
        vin[0, k] = item_v[k * width:(k + 1) * width, :].T
    pl.semaphore_wait(barrier, 2)

    def grad_step(col, k, v_now):
        half = v_now.astype(BF16)
        for row in range(0, users, ROWS):
            rows = slice(row, row + ROWS)
            cols = slice(k * width, (k + 1) * width)
            approx = dot_nn(user_h[rows, :], half)
            err = jnp.where(seen_v[col, rows, cols] != 0, approx - rate_v[col, rows, cols], 0.0).astype(BF16)
            err_v[rows, :] = err
            part = dot_nt(err, half)
            if k == 0:
                grad_u[rows, :] = part
            else:
                grad_u[rows, :] += part
        grad_v = dot_nn(user_t[...], err_v[...])
        return v_now - eta * (grad_v + lam * v_now)

    def level(sweep, carry):
        col = lax.rem(me + sweep, group)
        twice = steps_ref[0, col] > 1

        @pl.when(sweep < group)
        def _():
            for copy in load(sweep):
                copy.wait()

        @pl.when(sweep + 1 < group)
        def _():
            for copy in load(sweep + 1):
                copy.start()

        for k in range(CHUNKS):
            @pl.when(sweep > 0)
            def _():
                hop(sweep - 1, k).wait_recv()

            v_mid[k] = grad_step(col, k, vin[sweep, k])
        user_now = user_v[...]
        put_user(user_now - eta * (grad_u[...] + lam * user_now))
        for k in range(CHUNKS):
            v_now = v_mid[k]
            v_new = grad_step(col, k, v_now)
            vout[sweep, k] = jnp.where(twice, v_new, v_now)
            hop(sweep, k).start()
        user_now = user_v[...]
        user_new = user_now - eta * (grad_u[...] + lam * user_now)
        put_user(jnp.where(twice, user_new, user_now))
        return carry

    lax.fori_loop(0, levels, level, 0)

    user_out[...] = user_v[...]
    for k in range(CHUNKS):
        hop(levels - 1, k).wait_recv()
        item_out[k * width:(k + 1) * width, :] = vin[levels, k].T

    def drain(sweep, carry):
        for k in range(CHUNKS):
            hop(sweep, k).wait_send()
        return carry

    lax.fori_loop(0, levels, drain, 0)


def emit_kernel(user_v, item_v, user_out, item_out, sem):
    copies = (
        pltpu.make_async_copy(user_v, user_out, sem.at[0]),
        pltpu.make_async_copy(item_v, item_out, sem.at[1]),
    )
    for copy in copies:
        copy.start()
    for copy in copies:
        copy.wait()


def solution(mesh):
    axis = "shard"
    group = mesh.shape[axis]
    row_spec = P(("rep", axis), None)
    levels = EPOCHS * group

    def local_run(ratings, obs_mask, step_counts, user_init, item_init):
        users, rank = user_init.shape
        items = item_init.shape[0]
        width = items // CHUNKS
        vmem = pl.BlockSpec(memory_space=pltpu.VMEM)
        hbm = pl.BlockSpec(memory_space=pl.ANY)
        user_new, item_new = pl.pallas_call(
            functools.partial(sgd_kernel, group, axis),
            name="sgd",
            out_shape=(
                pltpu.VMEM((users, rank), F32),
                pltpu.VMEM((items, rank), F32),
            ),
            in_specs=[pl.BlockSpec(memory_space=pltpu.SMEM), hbm, hbm, hbm, hbm],
            out_specs=(vmem, vmem),
            scratch_shapes=[
                pltpu.VMEM((group, users, items), F32),
                pltpu.VMEM((group, users, items), jnp.int32),
                pltpu.VMEM((levels + 1, CHUNKS, rank, width), F32),
                pltpu.VMEM((levels, CHUNKS, rank, width), F32),
                pltpu.VMEM((CHUNKS, rank, width), F32),
                pltpu.VMEM((items, rank), F32),
                pltpu.VMEM((users, rank), F32),
                pltpu.VMEM((users, rank), BF16),
                pltpu.VMEM((rank, users), BF16),
                pltpu.VMEM((users, rank), F32),
                pltpu.VMEM((users, width), BF16),
                pltpu.SemaphoreType.DMA((group,)),
                pltpu.SemaphoreType.DMA((group,)),
                pltpu.SemaphoreType.DMA((levels, CHUNKS)),
                pltpu.SemaphoreType.DMA((levels, CHUNKS)),
                pltpu.SemaphoreType.DMA((2,)),
            ],
            compiler_params=pltpu.CompilerParams(
                collective_id=0, has_side_effects=True, vmem_limit_bytes=60 * 1024 * 1024
            ),
        )(step_counts, user_init, item_init, ratings, obs_mask)
        return pl.pallas_call(
            emit_kernel,
            name="emit",
            out_shape=(
                jax.ShapeDtypeStruct((users, rank), F32),
                jax.ShapeDtypeStruct((items, rank), F32),
            ),
            in_specs=[vmem, vmem],
            out_specs=(hbm, hbm),
            scratch_shapes=[pltpu.SemaphoreType.DMA((2,))],
        )(*(pltpu.with_memory_space_constraint(x, pltpu.VMEM) for x in (user_new, item_new)))

    return jax.shard_map(local_run, mesh=mesh, in_specs=(row_spec,) * 5, out_specs=(row_spec, row_spec), check_vma=False)
```
